256 devices in a mesh: blk: 32 (over x, z), col: 8 (over y, core).
Axes of the slice: x: 4, y: 4, z: 8, core: 2. Of those that a mesh axis runs over, the one named last changes fastest.
Arguments:
- momentum: float32 [8192, 29568], P('blk', 'col'), may hold values from -200 to 200
- grad: bfloat16 [8192, 29568], P('blk', 'col'), may hold values from -6 to 6
- q_basis: bfloat16 [1024, 29568], P('blk', 'col'), may hold values from -6 to 6
Outputs:
- momentum_new: float32 [8192, 29568], P('blk', 'col')
- update: bfloat16 [8192, 29568], P('blk', 'col')
- q_new: bfloat16 [1024, 29568], P('blk', 'col')
The draws below stay inside these ranges and needn't reach their ends.
All inputs are finite; a program needn't handle non-finite values.
Results may differ from the reference program's by a relative error of at most 0.022.
Values may be sent and summed in bfloat16 or wider, within the bound.
No kernel may reach another device: no remote copies, remote signals or barrier semaphores. Data moves between devices by JAX's collectives and lax.ppermute only.
A program may use at most 128 MiB of HBM per device.

```python
import jax
import jax.numpy as jnp
from jax import lax

FF = 29568
RANK = 1024
D_MODEL = 8192
N_BLK = 32
N_COL = 8


def draw_momentum(key, part):
    keys = jax.random.split(jax.random.fold_in(key, 11), 3)
    base = jax.random.truncated_normal(keys[0], -6.0, 6.0, (D_MODEL, FF), jnp.float32)
    row_rise = 0.5 + jnp.arange(D_MODEL, dtype=jnp.float32) / (D_MODEL - 1)
    row_spread = jnp.exp(jax.random.uniform(keys[1], (D_MODEL, 1), jnp.float32, -1.1513, 1.1513))
    col_spread = jnp.exp(jax.random.uniform(keys[2], (1, FF), jnp.float32, -1.1513, 1.1513))
    field = base * row_rise[:, None] * row_spread * col_spread
    return jnp.clip(field, -200.0, 200.0)


def block_levels(key, extent, cuts, least, largest):
    def one(position, blocks):
        draws = jax.random.uniform(jax.random.fold_in(jax.random.fold_in(key, 6), position), (blocks,), jnp.float32, least / len(cuts), largest / len(cuts))
        return jnp.repeat(jnp.exp(draws), extent[position] // blocks).reshape((-1,) + (1,) * (len(extent) - position - 1))

    loudness = one(*cuts[0])
    for cut in cuts[1:]:
        loudness = loudness * one(*cut)
    return loudness


def scatter_about(own_key, extent, spread, most, pieces=(), kind=jnp.bfloat16):
    factor_of = block_levels(own_key, extent, pieces, -0.22, 0.18) if pieces else 1.0
    result = jax.random.normal(own_key, extent, jnp.float32) * spread * factor_of
    return jnp.minimum(jnp.maximum(result, -most), most).astype(kind)


def setup_inputs(seed: int = 0) -> dict:
    arg_keys = jax.random.split(jax.random.key(seed), 4)
    return {
        "momentum": draw_momentum(jax.random.fold_in(arg_keys[3], 71), 0),
        "grad": scatter_about(arg_keys[1], (D_MODEL, FF), 1.0, 6.0, ((0, 32), (1, 8))),
        "q_basis": scatter_about(arg_keys[2], (RANK, FF), 1.0, 6.0, ((0, 32), (1, 8))),
    }


decay_rest = 0.05
epsilon = 1e-06

def reference(momentum, grad, q_basis):
    rows_total = momentum.shape[0]
    feature_count = momentum.shape[1]
    rank_count = q_basis.shape[0]
    b_matrix = momentum + grad.astype(jnp.float32)
    b_half = b_matrix.astype(jnp.bfloat16)
    col_width = feature_count // N_COL

    def p_step(index, running):
        start = (index * col_width).astype(jnp.int32)
        b_slice = lax.dynamic_slice_in_dim(b_half, start, col_width, 1)
        q_slice = lax.dynamic_slice_in_dim(q_basis, start, col_width, 1)
        partial_value = lax.dot_general(b_slice, q_slice, (((1,), (1,)), ((), ())), preferred_element_type=jnp.float32)
        rounded = lax.optimization_barrier(partial_value.astype(jnp.bfloat16))
        return running + rounded.astype(jnp.float32)
    p_matrix = lax.fori_loop(0, N_COL, p_step, jnp.zeros((rows_total, rank_count), jnp.float32))
    p_scale = jnp.sqrt(lax.optimization_barrier(jnp.sum(p_matrix * p_matrix, axis=0)) / rows_total + epsilon)
    p_hat = (p_matrix / p_scale[None, :]).astype(jnp.bfloat16)
    row_height = rows_total // N_BLK

    def r_step(index, running):
        start = (index * row_height).astype(jnp.int32)
        p_slice = lax.dynamic_slice_in_dim(p_hat, start, row_height, 0)
        b_slice = lax.dynamic_slice_in_dim(b_half, start, row_height, 0)
        partial_value = lax.dot_general(p_slice, b_slice, (((0,), (0,)), ((), ())), preferred_element_type=jnp.float32)
        rounded = lax.optimization_barrier(partial_value.astype(jnp.bfloat16))
        return running + rounded.astype(jnp.float32)
    r_matrix = lax.fori_loop(0, N_BLK, r_step, jnp.zeros((rank_count, feature_count), jnp.float32))
    r_scale = jnp.sqrt(lax.optimization_barrier(jnp.sum(r_matrix * r_matrix, axis=1)) / feature_count + epsilon)
    q_new = (r_matrix / r_scale[:, None]).astype(jnp.bfloat16)
    weighted = (p_hat.astype(jnp.float32) * (decay_rest * r_scale / rows_total)[None, :]).astype(jnp.bfloat16)
    update_sum = jnp.dot(p_hat, q_new, preferred_element_type=jnp.float32)
    correction = jnp.dot(weighted, q_new, preferred_element_type=jnp.float32)
    update = (update_sum * (1.0 / jnp.sqrt(jnp.float32(rank_count)))).astype(jnp.bfloat16)
    return (b_matrix - correction, update, q_new)
```

```python
import jax
import jax.numpy as jnp
from jax import lax
from jax.experimental import pallas as pl
from jax.experimental.pallas import tpu as pltpu
from jax.sharding import Mesh
from jax.sharding import PartitionSpec as P


decay_rest = 0.05
epsilon = 1e-06
X, Z, Y, C = 4, 8, 4, 2
f32, bf16 = jnp.float32, jnp.bfloat16
VMEM = pl.BlockSpec(memory_space=pltpu.VMEM)
SMEM = pl.BlockSpec(memory_space=pltpu.SMEM)


def shift(x, axis, by):
    n = lax.axis_size(axis)
    return lax.ppermute(x, axis, [(i, (i + by) % n) for i in range(n)])


def ring_gather(own, n, axis):
    half = own.shape[0] // 2
    blocks = {0: own}
    low, high = own, own
    for step in range(1, n // 2):
        low = shift(low, axis, 1)
        high = shift(high, axis, -1)
        blocks[n - step] = low
        blocks[step] = high
    first = shift(low[:half], axis, 1)
    second = shift(high[half:], axis, -1)
    blocks[n // 2] = (first, second)
    return blocks


def nt(a, b):
    return lax.dot_general(a, b, (((1,), (1,)), ((), ())), preferred_element_type=f32)


def nn(a, b):
    return lax.dot_general(a, b, (((1,), (0,)), ((), ())), preferred_element_type=f32)


def p_kernel(s_ref, *refs):
    q_refs, b_refs = refs[:9], refs[9:13]
    send_ref, keep_ref = refs[13:]
    x, c = s_ref[0], s_ref[2]
    rows = q_refs[0].shape[0]

    def half(h, out):
        for k in range(X):
            b = b_refs[k][...]
            for j in range(4):
                ch = 4 * h + j
                if ch < 4:
                    q = q_refs[ch][...]
                elif ch == 4:
                    q = jnp.concatenate([q_refs[4][...], q_refs[5][...]], axis=0)
                else:
                    q = q_refs[ch + 1][...]
                out[lax.rem(x + k, X), pl.ds(j * rows, rows), :] = nn(q, b).astype(bf16)

    @pl.when(c == 0)
    def _():
        half(1, send_ref)
        half(0, keep_ref)

    @pl.when(c == 1)
    def _():
        half(0, send_ref)
        half(1, keep_ref)


def r_kernel(s_ref, *refs):
    b_refs, mine, other = refs[:4], refs[4], refs[5]
    out_refs, sq_ref = refs[6:14], refs[14]
    x, c = s_ref[0], s_ref[2]
    for j in (4, 3, 5, 2, 6, 1, 7, 0):
        acc = None
        total = None
        for k in range(X):
            a = lax.rem(x + k, X)
            p = jnp.where(c == j // 4, mine[a, j % 4], other[a, j % 4])
            part = nt(b_refs[k][...], p)
            acc = part if acc is None else acc + part
            pf = p.astype(f32)
            sq = pf * pf
            total = sq if total is None else total + sq
        out_refs[j][...] = acc.astype(bf16)
        sums = jnp.sum(total, axis=1, keepdims=True)
        sq_ref[j] = jnp.transpose(jnp.broadcast_to(sums, (128, 128)))[:8]


def final_kernel(s_ref, mom, grad, mine, other, fu, fc, fq, *refs):
    na = 8 + 1
    a_own = refs[:na]
    a_far = [refs[na + 3 * i : na + 3 * i + 3] for i in range(3)]
    b_parts = refs[na + 9 : na + 18]
    new_ref, upd_ref, q_ref, w_ref = refs[na + 18 :]
    k = pl.program_id(0)
    x, c = s_ref[0], s_ref[2]
    h = a_own[0].shape[0]

    @pl.when(k == 0)
    def _():
        for j in range(8):
            p = jnp.where(c == j // 4, mine[0, j % 4], other[0, j % 4]).astype(f32)
            rows = pl.ds(128 * j, 128)
            u = jnp.concatenate([fu[rows, :]] * 2, axis=1)
            w = jnp.concatenate([fc[rows, :]] * 2, axis=1)
            w_ref[rows, :256] = (p * u).astype(bf16)
            w_ref[rows, 256:] = (p * w).astype(bf16)

    groups = {0: (0, 0), 1: (0, 1), 7: (0, 2), 2: (1, 0), 6: (1, 1), 3: (2, 0), 5: (2, 1), 4: (2, 2)}
    for kk in range(X):

        @pl.when(k == kk)
        def _():
            for part in range(2):
                cols = []
                for j in range(8):
                    if part == 0:
                        if kk == 0:
                            if j < 4:
                                cols.append(a_own[j][...])
                            elif j == 4:
                                cols.append(jnp.concatenate([a_own[4][...], a_own[5][...]], axis=0))
                            else:
                                cols.append(a_own[j + 1][...])
                        else:
                            g, i = groups[j]
                            cols.append(a_far[kk - 1][g][pl.ds(i * h, h), :])
                    else:
                        if j < 4:
                            cols.append(b_parts[j][pl.ds(kk * h, h), :])
                        elif j == 4:
                            cols.append(b_parts[4 + kk // 2][pl.ds((kk % 2) * h, h), :])
                        else:
                            cols.append(b_parts[j + 1][pl.ds(kk * h, h), :])
                left = jnp.concatenate(cols, axis=1)
                out = nn(left, w_ref[...])
                rows = pl.ds(part * h, h)
                upd_ref[rows, :] = out[:, :256].astype(bf16)
                b = mom[rows, :] + grad[rows, :].astype(f32)
                new_ref[rows, :] = b - out[:, 256:]
                q = cols[0].astype(f32) * fq[0:1, :]
                turned = jnp.transpose(q)
                pick = turned[0:32]
                for i in range(1, X):
                    pick = jnp.where(x == i, turned[32 * i : 32 * i + 32], pick)
                q_ref[0, part] = pick.astype(bf16)


def shards(momentum, grad, q_basis):
    xi, zi, yi, ci = (lax.axis_index(a) for a in ("x", "z", "y", "c"))
    where = jnp.stack([xi, zi, ci]).astype(jnp.int32)
    mt, gt = momentum.T, grad.T
    n, rows = mt.shape
    n_rank = q_basis.shape[0]
    w = -(-n // (X * 16)) * 16
    rows_total = rows * X * Z
    feature_count = n * Y * C

    qp = jnp.pad(q_basis, ((0, 0), (0, X * w - n))).reshape(n_rank, X, w).transpose(1, 0, 2)
    q0 = lax.all_to_all(qp, "x", 0, 0, tiled=True).reshape(X * n_rank, w)
    bt = (mt + gt.astype(f32)).astype(bf16)
    bt, q0 = lax.optimization_barrier((bt, q0))
    qr = ring_gather(q0, Z, "z")

    bt = jnp.pad(bt, ((0, X * w - n), (0, 0))).reshape(X, w, rows)
    cut = [lax.dynamic_index_in_dim(bt, lax.rem(xi + k, X), 0, keepdims=False) for k in range(X)]
    b_rel = [cut[0], shift(cut[3], "x", -1), shift(cut[2], "x", 2), shift(cut[1], "x", 1)]

    qs = [qr[0], qr[1], qr[2], qr[3], qr[4][0], qr[4][1], qr[5], qr[6], qr[7]]
    ranks = X * n_rank
    half_shape = jax.ShapeDtypeStruct((X, 4 * ranks, rows), bf16)
    send, keep = pl.pallas_call(
        p_kernel,
        out_shape=(half_shape, half_shape),
        in_specs=[SMEM] + [VMEM] * 13,
        out_specs=(VMEM, VMEM),
        name="p_kernel",
        cost_estimate=pl.CostEstimate(flops=2 * 1024 * 1024 * w, bytes_accessed=6_000_000, transcendentals=0),
    )(where, *qs, *b_rel)
    got = shift(send, "c", 1)
    both = (keep.astype(f32) + got.astype(f32)).astype(bf16).reshape(X * Y, ranks, rows)
    pieces = lax.all_to_all(both, ("x", "y"), 0, 0, tiled=True)
    p_own = pieces.astype(f32).sum(axis=0).astype(bf16)
    copies = jnp.broadcast_to(p_own, (X * Y, ranks, rows))
    mine = lax.all_to_all(copies, ("x", "y"), 0, 0, tiled=True).reshape(X, Y, ranks, rows)
    other = shift(mine, "c", 1)

    outs = pl.pallas_call(
        r_kernel,
        out_shape=tuple([jax.ShapeDtypeStruct((w, ranks), bf16)] * 8 + [jax.ShapeDtypeStruct((8, 8, ranks), f32)]),
        in_specs=[SMEM] + [VMEM] * 6,
        out_specs=tuple([VMEM] * 9),
        name="r_kernel",
        cost_estimate=pl.CostEstimate(flops=2 * 1024 * 1024 * w, bytes_accessed=6_000_000, transcendentals=0),
    )(where, *b_rel, mine, other)
    parts, sq = outs[:8], outs[8][:, 0, :]

    h = w // 2
    add = lambda a, b: (a.astype(f32) + b.astype(f32))
    right = shift(parts[4][:h], "z", 1)
    left = shift(parts[4][h:], "z", -1)
    right = shift(jnp.concatenate([add(right, parts[3][:h]).astype(bf16), parts[3][h:]]), "z", 1)
    left = shift(jnp.concatenate([parts[5][:h], add(left, parts[5][h:]).astype(bf16)]), "z", -1)
    right = shift(add(right, parts[2]).astype(bf16), "z", 1)
    left = shift(add(left, parts[6]).astype(bf16), "z", -1)
    right = shift(add(right, parts[1]).astype(bf16), "z", 1)
    left = shift(add(left, parts[7]).astype(bf16), "z", -1)
    r_sum = add(right, left) + parts[0].astype(f32)
    r_own = r_sum.astype(bf16)

    sq2 = jnp.concatenate([sq, sq], axis=0)
    to_owner = lax.dynamic_slice_in_dim(sq2, lax.rem(Z - zi, Z), Z, 0)
    sq_own = lax.all_to_all(to_owner, "z", 0, 0, tiled=True).sum(axis=0)
    p_var = sq_own / rows_total + epsilon
    r_sq = jnp.sum(r_sum * r_sum, axis=0)
    r_sq = lax.all_to_all(jnp.broadcast_to(r_sq, (X * Y * C, ranks)), ("x", "y", "c"), 0, 0, tiled=True).sum(axis=0)
    r_var = r_sq / p_var / feature_count + epsilon
    scales = jnp.stack([p_var, r_var])
    scales = lax.all_to_all(jnp.broadcast_to(scales, (Z, 2, ranks)), "z", 0, 0, tiled=True)
    s2 = jnp.concatenate([scales, scales], axis=0)
    rel = lax.dynamic_slice_in_dim(s2, zi, Z, 0)
    p_var_all, r_scale_all = rel[:, 0].reshape(-1), jnp.sqrt(rel[:, 1]).reshape(-1)
    fu = (1.0 / jnp.sqrt(f32(Z * ranks))) / (p_var_all * r_scale_all)
    fc = (decay_rest / rows_total) / p_var_all
    fq = jnp.broadcast_to((1.0 / (jnp.sqrt(p_var) * jnp.sqrt(r_var)))[None], (8, ranks))
    fu = jnp.broadcast_to(fu[:, None], (Z * ranks, 128))
    fc = jnp.broadcast_to(fc[:, None], (Z * ranks, 128))

    top, low = r_own[:h], r_own[h:]
    low_x = jnp.concatenate([low, shift(low, "x", -1), shift(low, "x", 2), shift(low, "x", 1)])
    a = ring_gather(top, Z, "z")
    a[4] = jnp.concatenate(a[4])
    groups = [jnp.concatenate([a[0], a[1], a[7]]), jnp.concatenate([a[2], a[6]]), jnp.concatenate([a[3], a[5], a[4]])]
    far = []
    for by in (-1, 2, 1):
        far += [shift(g, "x", by) for g in groups]
    b = ring_gather(low_x, Z, "z")
    bs = [b[0], b[1], b[2], b[3], b[4][0], b[4][1], b[5], b[6], b[7]]
    a_own = [a[0], a[1], a[2], a[3], a[4][: h // 2], a[4][h // 2 :], a[5], a[6], a[7]]

    wide = lambda k, s: (lax.rem(s[0] + k, X), 0)
    one = lambda k, s: (s[0], 0, 0, 0)
    new_t, upd_t, q_parts = pl.pallas_call(
        final_kernel,
        grid_spec=pltpu.PrefetchScalarGridSpec(
            num_scalar_prefetch=1,
            grid=(X,),
            in_specs=[
                pl.BlockSpec((w, rows), wide),
                pl.BlockSpec((w, rows), wide),
                pl.BlockSpec((1, Y, ranks, rows), one),
                pl.BlockSpec((1, Y, ranks, rows), one),
            ]
            + [VMEM] * (3 + 9 + 9 + 9),
            out_specs=(
                pl.BlockSpec((w, rows), wide),
                pl.BlockSpec((w, rows), wide),
                pl.BlockSpec((1, 2, n_rank, h), lambda k, s: (lax.rem(s[0] + k, X), 0, 0, 0)),
            ),
            scratch_shapes=[pltpu.VMEM((Z * ranks, 2 * rows), bf16)],
        ),
        out_shape=(
            jax.ShapeDtypeStruct((n, rows), f32),
            jax.ShapeDtypeStruct((n, rows), bf16),
            jax.ShapeDtypeStruct((X, 2, n_rank, h), bf16),
        ),
        name="final_kernel",
        compiler_params=pltpu.CompilerParams(vmem_limit_bytes=56 * 1024 * 1024),
        cost_estimate=pl.CostEstimate(flops=4 * 256 * 1024 * n, bytes_accessed=20_000_000, transcendentals=0),
    )(where, mt, gt, mine, other, fu, fc, fq, *a_own, *far, *bs)
    q_new = q_parts.transpose(2, 0, 1, 3).reshape(n_rank, X * w)[:, :n]
    return new_t.T, upd_t.T, q_new


def solution(mesh):
    grid = Mesh(mesh.devices.reshape(X, Z, Y, C), ("x", "z", "y", "c"))
    spec = P(("x", "z"), ("y", "c"))
    return jax.shard_map(shards, mesh=grid, in_specs=(spec,) * 3, out_specs=(spec,) * 3, check_vma=False)
```
